32 devices in a mesh: wide: 8 (over y, x, core), narrow: 4 (over z).
Axes of the slice: x: 2, y: 2, z: 4, core: 2. Of those that a mesh axis runs over, the one named last changes fastest.
Arguments:
- tokens: bfloat16 [16, 1184, 1024], P('wide', 'narrow'), may hold values from -6 to 6
- timestep: bfloat16 [16, 1024], P('wide'), may hold values from -6 to 6
- context: int32 [16, 2], P('wide'), may hold values from 0 to 475
- w_qkv: bfloat16 [1024, 3, 1024], P('wide', None, 'narrow'), may hold values from -0.1875 to 0.1875
- w_out: bfloat16 [1024, 1024], P('narrow', 'wide'), may hold values from -1.5 to 1.5
- w_up: bfloat16 [1024, 4096], P('wide', 'narrow'), may hold values from -0.1875 to 0.1875
- w_down: bfloat16 [4096, 1024], P('narrow', 'wide'), may hold values from -0.09375 to 0.09375
- b_up: bfloat16 [4096], P(('wide', 'narrow')), may hold values from -3 to 3
- biases: bfloat16 [6, 1024], P(None, ('wide', 'narrow')), may hold values from -3 to 3
- gains: bfloat16 [2, 1024], P(None, ('wide', 'narrow')), may hold values from 0.25 to 1.75
- cotangent: bfloat16 [16, 1184, 1024], P('wide', 'narrow'), may hold values from -6 to 6
Outputs:
- output: bfloat16 [16, 1184, 1024], P('wide', 'narrow')
- grad_tokens: float32 [16, 1184, 1024], P('wide', 'narrow')
- grad_qkv: float32 [1024, 3, 1024], P('wide', None, 'narrow')
- grad_out: float32 [1024, 1024], P('narrow', 'wide')
- grad_up: float32 [1024, 4096], P('wide', 'narrow')
- grad_down: float32 [4096, 1024], P('narrow', 'wide')
- grad_b_up: float32 [4096], P(('wide', 'narrow'))
- grad_biases: float32 [6, 1024], P(None, ('wide', 'narrow'))
- grad_gains: float32 [2, 1024], P(None, ('wide', 'narrow'))
The draws below stay inside these ranges and needn't reach their ends.
All inputs are finite; a program needn't handle non-finite values.
Results may differ from the reference program's by a relative error of at most 0.018.
Values may be sent and summed in bfloat16 or wider, within the bound.
A program may use at most 256 MiB of HBM per device.

```python
import jax
import jax.numpy as jnp
from jax import lax

D = 1024
HEADS = 16
HEAD_DIM = 64
FF = 4096
ITEM = 592
NOISE = 25
CTX = 475
SEQ = 1184
ROWS = 16


def place_ends(values, key, least, high):
    shape = values.shape
    index_at = [jax.random.randint(jax.random.fold_in(key, axis), (), 0, shape[axis]) for axis in range(len(shape))]
    values = values.at[tuple(index_at)].set(least)
    longest = shape.index(max(shape))
    index_at[longest] = (index_at[longest] + 1) % shape[longest]
    return values.at[tuple(index_at)].set(high)


def block_scale(own_key, dims, shards, smallest, top_value):
    factor_of = 1.0
    for dim, parts in shards:
        steps = jax.random.uniform(jax.random.fold_in(jax.random.fold_in(own_key, 6), dim), (parts,), jnp.float32, smallest / len(shards), top_value / len(shards))
        factor_of = factor_of * jnp.repeat(jnp.exp(steps), dims[dim] // parts).reshape((-1,) + (1,) * (len(dims) - 1 - dim))
    return factor_of


def centred(rng, dims, scale, limit, shards=(), kind=jnp.bfloat16):
    values = jax.random.normal(rng, dims, jnp.float32) * scale
    if len(shards) > 0:
        values = block_scale(rng, dims, shards, -0.22, 0.18) * values
    return jnp.clip(values, min=-limit, max=limit).astype(kind)


def setup_inputs(seed: int = 0) -> dict:
    keys = jax.random.split(jax.random.key(seed), 12)
    tokens = centred(keys[0], (ROWS, SEQ, D), 1.0, 6.0, ((0, 8), (1, 4)))
    timestep = centred(keys[1], (ROWS, D), 1.0, 6.0, ((0, 8),))
    context = place_ends(jax.random.randint(keys[2], (ROWS, 2), 0, CTX + 1), jax.random.fold_in(keys[2], 1), 0, CTX).astype(jnp.int32)
    w_qkv = centred(keys[3], (D, 3, D), D ** -0.5, 0.1875, ((0, 8), (2, 4)))
    w_out = centred(keys[4], (D, D), 16 ** -0.5, 1.5, ((0, 4), (1, 8)))
    w_up = centred(keys[5], (D, FF), D ** -0.5, 0.1875, ((0, 8), (1, 4)))
    w_down = centred(keys[6], (FF, D), FF ** -0.5, 0.09375, ((0, 4), (1, 8)))
    b_up = centred(keys[7], (FF,), 0.5, 3.0, ((0, 32),))
    biases = centred(keys[8], (6, D), 0.5, 3.0, ((1, 32),))
    gains = jnp.clip(1.0 + 0.15 * jax.random.normal(keys[9], (2, D), jnp.float32), 0.25, 1.75).astype(jnp.bfloat16)
    cotangent = centred(keys[10], (ROWS, SEQ, D), 1.0, 6.0, ((0, 8), (1, 4)))
    return dict(tokens=tokens, timestep=timestep, context=context, w_qkv=w_qkv, w_out=w_out, w_up=w_up, w_down=w_down, b_up=b_up, biases=biases, gains=gains, cotangent=cotangent)


highest = lax.Precision.HIGHEST

@jax.custom_vjp
def low(v):
    return lax.optimization_barrier(v.astype(jnp.bfloat16)).astype(jnp.float32)

@jax.custom_vjp
def low_back(v):
    return v

def low_keep(v):
    return (low(v), None)

def low_pass(kept, grad):
    return (grad,)

def back_keep(v):
    return (v, None)

def back_low(kept, grad):
    return (low(grad),)
low.defvjp(low_keep, low_pass)
low_back.defvjp(back_keep, back_low)

def positions(context_row):
    position = jnp.arange(SEQ, dtype=jnp.int32)
    item_index = position // ITEM
    offset = position - item_index * ITEM
    item_start = jnp.where(item_index == 0, context_row[0], context_row[1])
    noisy_mask = (offset >= item_start) & (offset < item_start + NOISE)
    key_valid = offset < item_start + NOISE
    same_item = item_index[:, None] == item_index[None, :]
    return (noisy_mask, same_item & key_valid[None, :])

def layer_norm(hidden, gain_vec, shift_vec):
    center = hidden - lax.optimization_barrier(jnp.mean(hidden, -1, keepdims=True))
    spread = lax.optimization_barrier(jnp.mean(center * center, -1, keepdims=True))
    return center * lax.rsqrt(spread + 1e-05) * gain_vec + shift_vec

def layer(token_row, embed_row, weights, noisy_mask, key_valid):
    w_qkv, w_out, w_up, w_down, b_up, biases, gains = weights
    xfull = token_row + jnp.where(noisy_mask[:, None], embed_row[None, :], 0.0)
    x_low = low(xfull)
    projected = jnp.einsum('sd,dcf->csf', x_low, w_qkv, precision=highest)
    queries = low(low_back(projected[0]) + biases[0]).reshape(SEQ, HEADS, HEAD_DIM)
    key_rows = low(low_back(projected[1])).reshape(SEQ, HEADS, HEAD_DIM)
    value_rows = low(low_back(projected[2]) + biases[1]).reshape(SEQ, HEADS, HEAD_DIM)
    scores = jnp.einsum('qhe,khe->hqk', queries, key_rows, precision=highest) * HEAD_DIM ** (-0.5)
    scores = jnp.where(key_valid[None, :, :], low_back(scores), -jnp.inf)
    probs = jax.nn.softmax(scores, axis=-1)
    attended = jnp.einsum('hqk,khe->qhe', low(probs), value_rows, precision=highest).reshape(SEQ, D)
    attended = low(low_back(attended))
    first_sum = xfull + low_back(jnp.dot(attended, w_out, precision=highest)) + biases[2]
    first_norm = layer_norm(first_sum, gains[0], biases[4])
    pre_act = low_back(jnp.dot(low(first_norm), w_up, precision=highest)) + b_up
    activated = low(jax.nn.gelu(pre_act, approximate=False))
    second_sum = first_norm + low_back(jnp.dot(activated, w_down, precision=highest)) + biases[3]
    return layer_norm(second_sum, gains[1], biases[5])

def reference(tokens, timestep, context, w_qkv, w_out, w_up, w_down, b_up, biases, gains, cotangent):
    weights = tuple((w.astype(jnp.float32) for w in (w_qkv, w_out, w_up, w_down, b_up, biases, gains)))

    def step_row(totals, inputs):
        token_row, embed_row, context_row, cot_row = inputs
        noisy_mask, key_valid = positions(context_row)
        embed_f = embed_row.astype(jnp.float32)

        def forward(tok_in, weight_in):
            return layer(tok_in, embed_f, weight_in, noisy_mask, key_valid)
        result, pullback = jax.vjp(forward, token_row.astype(jnp.float32), weights)
        grad_row, grad_weights = pullback(cot_row.astype(jnp.float32))
        totals = jax.tree.map(jnp.add, totals, grad_weights)
        return (totals, (result.astype(jnp.bfloat16), grad_row))
    start_totals = tuple((jnp.zeros(w.shape, jnp.float32) for w in weights))
    totals, (output, grad_tokens) = lax.scan(step_row, start_totals, (tokens, timestep, context, cotangent))
    return (output, grad_tokens, totals[0], totals[1], totals[2], totals[3], totals[4], totals[5], totals[6])
```

```python
from functools import partial

import jax
import jax.numpy as jnp
from jax import lax
from jax.sharding import PartitionSpec as P

HEAD_DIM = 64
ITEM = 592
NOISE = 25
MB = 2
KEYS = 512
PAIRS = ((0, 1), (1, 0), (2, 3), (3, 2))


def spread_rows(piece):
    return lax.all_gather(piece, "narrow", axis=1, tiled=True)


def collect_sums(term):
    return lax.psum_scatter(
        term.astype(jnp.bfloat16), "narrow", scatter_dimension=1, tiled=True
    ).astype(jnp.float32)


def fetch_weights(w_qkv, w_out, w_up, w_down):
    full_qkv, full_out, full_up, full_down = (
        lax.all_gather(w_qkv, "wide", axis=0, tiled=True),
        lax.all_gather(w_out, "wide", axis=1, tiled=True),
        lax.all_gather(w_up, "wide", axis=0, tiled=True),
        lax.all_gather(w_down, "wide", axis=1, tiled=True),
    )
    whole_qkv, whole_out = (
        lax.all_gather(full_qkv, "narrow", axis=2, tiled=True),
        lax.all_gather(full_out, "narrow", axis=0, tiled=True),
    )
    return (whole_qkv, whole_out, full_up, full_down)


def reduce_grads(grad_set):
    return (
        lax.psum_scatter(
            grad_set[0].astype(jnp.bfloat16), "wide", scatter_dimension=0, tiled=True
        ).astype(jnp.float32),
        lax.psum_scatter(
            grad_set[1].astype(jnp.bfloat16), "wide", scatter_dimension=1, tiled=True
        ).astype(jnp.float32),
        lax.psum_scatter(
            grad_set[2].astype(jnp.bfloat16), "wide", scatter_dimension=0, tiled=True
        ).astype(jnp.float32),
        lax.psum_scatter(
            grad_set[3].astype(jnp.bfloat16), "wide", scatter_dimension=1, tiled=True
        ).astype(jnp.float32),
    )


def norm_forward(hidden, gain_vec, shift_vec):
    center = hidden - jnp.mean(hidden, -1, keepdims=True)
    inverse = lax.rsqrt(jnp.mean(center * center, -1, keepdims=True) + 1e-05)
    normed = center * inverse
    return (normed * gain_vec + shift_vec, normed, inverse)


def norm_backward(upstream, normed, inverse, gain_vec):
    scaled = upstream * gain_vec
    return inverse * (
        scaled
        - jnp.mean(scaled, -1, keepdims=True)
        - normed * jnp.mean(scaled * normed, -1, keepdims=True)
    )


def masked_scores(queries, key_rows, key_valid):
    scores = jnp.einsum("qhe,khe->hqk", queries, key_rows, preferred_element_type=jnp.float32)
    scores = scores * queries.shape[-1] ** (-0.5)
    item_index = jnp.arange(queries.shape[0], dtype=jnp.int32) // ITEM
    allowed = (item_index[:, None] == item_index[None, :]) & key_valid[None, :]
    return jnp.where(allowed[None, :, :], scores, -jnp.inf)


def attend_row(inputs):
    queries, key_rows, value_rows, key_valid = inputs
    scores = masked_scores(queries, key_rows, key_valid)
    top_score = jnp.max(scores, -1, keepdims=True)
    log_total = top_score + jnp.log(jnp.sum(jnp.exp(scores - top_score), -1, keepdims=True))
    probs_low = jnp.exp(scores - log_total).astype(jnp.bfloat16)
    attended = jnp.einsum("hqk,khe->qhe", probs_low, value_rows, preferred_element_type=jnp.float32)
    return (attended.reshape(attended.shape[0], -1).astype(jnp.bfloat16), log_total)


def attend_back(inputs):
    queries, key_rows, value_rows, key_valid, log_total, d_att = inputs
    probs = jnp.exp(masked_scores(queries, key_rows, key_valid) - log_total)
    probs_low = probs.astype(jnp.bfloat16)
    d_prob = jnp.einsum("qhe,khe->hqk", d_att, value_rows, preferred_element_type=jnp.float32)
    d_score = probs * (d_prob - jnp.sum(probs * d_prob, -1, keepdims=True))
    d_score_low = d_score.astype(jnp.bfloat16)
    factor = queries.shape[-1] ** (-0.5)
    d_queries = (
        jnp.einsum("hqk,khe->qhe", d_score_low, key_rows, preferred_element_type=jnp.float32)
        * factor
    )
    d_keys = (
        jnp.einsum("hqk,qhe->khe", d_score_low, queries, preferred_element_type=jnp.float32)
        * factor
    )
    d_values = jnp.einsum("hqk,qhe->khe", probs_low, d_att, preferred_element_type=jnp.float32)
    return (d_queries, d_keys, d_values)


def shards(tokens, timestep, context, w_qkv, w_out, w_up, w_down, b_up, biases, gains, cotangent):
    narrow_count = lax.axis_size("narrow")
    narrow_index = lax.axis_index("narrow")
    rows_here, piece_len, model_width = tokens.shape
    seq_len = piece_len * narrow_count
    local_width = w_qkv.shape[2]
    local_hidden = w_up.shape[1]
    heads_here = local_width // HEAD_DIM
    batch_rows = rows_here // MB
    bias_all, gain_all, up_bias_all = (
        lax.all_gather(biases, ("wide", "narrow"), axis=1, tiled=True),
        lax.all_gather(gains, ("wide", "narrow"), axis=1, tiled=True),
        lax.all_gather(b_up, ("wide", "narrow"), axis=0, tiled=True),
    )
    bias_all = bias_all.astype(jnp.float32)
    gain_all = gain_all.astype(jnp.float32)
    up_bias_all = up_bias_all.astype(jnp.float32)
    query_bias = lax.dynamic_slice_in_dim(bias_all[0], narrow_index * local_width, local_width)
    value_bias = lax.dynamic_slice_in_dim(bias_all[1], narrow_index * local_width, local_width)
    up_bias = lax.dynamic_slice_in_dim(up_bias_all, narrow_index * local_hidden, local_hidden)
    position = jnp.arange(seq_len, dtype=jnp.int32)
    item_index = position // ITEM
    offset = position - item_index * ITEM
    item_start = jnp.where(item_index[None, :] == 0, context[:, 0:1], context[:, 1:2])
    noisy_mask = (offset[None, :] >= item_start) & (offset[None, :] < item_start + NOISE)
    key_valid = offset[None, :] < item_start + NOISE
    noisy_here = lax.dynamic_slice_in_dim(noisy_mask, narrow_index * piece_len, piece_len, 1)
    grad_shares = None
    zero_width = jnp.zeros((model_width,), jnp.float32)
    sum_query_bias = jnp.zeros((local_width,), jnp.float32)
    sum_value_bias = jnp.zeros((local_width,), jnp.float32)
    sum_up_bias = jnp.zeros(up_bias.shape, jnp.float32)
    sum_out_bias = zero_width
    sum_down_bias = zero_width
    sum_shift_one = zero_width
    sum_shift_two = zero_width
    sum_gain_one = zero_width
    sum_gain_two = zero_width
    output_parts = []
    grad_parts = []
    head_shape = (batch_rows, seq_len, heads_here, HEAD_DIM)
    for batch in range(MB):
        row_range = slice(batch * batch_rows, (batch + 1) * batch_rows)
        token_part = tokens[row_range].astype(jnp.float32)
        embed_part = timestep[row_range].astype(jnp.float32)
        valid_part = key_valid[row_range]
        x_here = token_part + jnp.where(
            noisy_here[row_range][:, :, None], embed_part[:, None, :], 0.0
        )
        whole_qkv, whole_out, full_up, full_down = fetch_weights(w_qkv, w_out, w_up, w_down)
        local_qkv = lax.dynamic_slice_in_dim(whole_qkv, narrow_index * local_width, local_width, 2)
        local_out = lax.dynamic_slice_in_dim(whole_out, narrow_index * local_width, local_width, 0)
        x_all = spread_rows(x_here.astype(jnp.bfloat16))
        projected = jnp.einsum(
            "rsd,dcf->crsf", x_all, local_qkv, preferred_element_type=jnp.float32
        )
        queries = (projected[0] + query_bias).astype(jnp.bfloat16).reshape(head_shape)
        key_rows = projected[1].astype(jnp.bfloat16).reshape(head_shape)
        value_rows = (projected[2] + value_bias).astype(jnp.bfloat16).reshape(head_shape)
        attended, log_total = lax.map(attend_row, (queries, key_rows, value_rows, valid_part))
        attended_here = lax.all_to_all(attended, "narrow", split_axis=1, concat_axis=2, tiled=True)
        first_sum = (
            x_here
            + jnp.einsum(
                "rsf,fd->rsd", attended_here, whole_out, preferred_element_type=jnp.float32
            )
            + bias_all[2]
        )
        first_norm, normed_one, inverse_one = norm_forward(first_sum, gain_all[0], bias_all[4])
        ffn_input = spread_rows(first_norm.astype(jnp.bfloat16))
        pre_act = (
            jnp.einsum("rsd,df->rsf", ffn_input, full_up, preferred_element_type=jnp.float32)
            + up_bias
        )
        activated, gelu_pull = jax.vjp(partial(jax.nn.gelu, approximate=False), pre_act)
        activated = activated.astype(jnp.bfloat16)
        down_term = jnp.einsum(
            "rsf,fd->rsd", activated, full_down, preferred_element_type=jnp.float32
        )
        second_sum = first_norm + collect_sums(down_term) + bias_all[3]
        result, normed_two, inverse_two = norm_forward(second_sum, gain_all[1], bias_all[5])
        output_parts.append(result.astype(jnp.bfloat16))
        cot_part = cotangent[row_range].astype(jnp.float32)
        sum_gain_two = sum_gain_two + jnp.sum(cot_part * normed_two, (0, 1))
        sum_shift_two = sum_shift_two + jnp.sum(cot_part, (0, 1))
        d_second = norm_backward(cot_part, normed_two, inverse_two, gain_all[1])
        sum_down_bias = sum_down_bias + jnp.sum(d_second, (0, 1))
        d_second_all = spread_rows(d_second.astype(jnp.bfloat16))
        grad_down = jnp.einsum(
            "rsf,rsd->fd", activated, d_second_all, preferred_element_type=jnp.float32
        )
        d_act = jnp.einsum(
            "rsd,fd->rsf", d_second_all, full_down, preferred_element_type=jnp.float32
        )
        d_pre = gelu_pull(d_act)[0]
        sum_up_bias = sum_up_bias + jnp.sum(d_pre, (0, 1))
        d_pre_low = d_pre.astype(jnp.bfloat16)
        grad_up = jnp.einsum(
            "rsd,rsf->df", ffn_input, d_pre_low, preferred_element_type=jnp.float32
        )
        back_term = jnp.einsum(
            "rsf,df->rsd", d_pre_low, full_up, preferred_element_type=jnp.float32
        )
        d_first_norm = d_second + collect_sums(back_term)
        sum_gain_one = sum_gain_one + jnp.sum(d_first_norm * normed_one, (0, 1))
        sum_shift_one = sum_shift_one + jnp.sum(d_first_norm, (0, 1))
        d_first = norm_backward(d_first_norm, normed_one, inverse_one, gain_all[0])
        sum_out_bias = sum_out_bias + jnp.sum(d_first, (0, 1))
        d_first_all = spread_rows(d_first.astype(jnp.bfloat16))
        grad_out = jnp.einsum(
            "rsf,rsd->fd", attended, d_first_all, preferred_element_type=jnp.float32
        )
        d_att = jnp.einsum(
            "rsd,fd->rsf", d_first_all, local_out, preferred_element_type=jnp.float32
        ).astype(jnp.bfloat16)
        d_queries, d_keys, d_values = lax.map(
            attend_back,
            (queries, key_rows, value_rows, valid_part, log_total, d_att.reshape(head_shape)),
        )
        flat_shape = (batch_rows, seq_len, local_width)
        d_queries = d_queries.reshape(flat_shape)
        d_keys = d_keys.reshape(flat_shape)
        d_values = d_values.reshape(flat_shape)
        sum_query_bias = sum_query_bias + jnp.sum(d_queries, (0, 1))
        sum_value_bias = sum_value_bias + jnp.sum(d_values, (0, 1))
        d_proj = jnp.stack([d_queries, d_keys, d_values]).astype(jnp.bfloat16)
        grad_qkv = jnp.einsum("rsd,crsf->dcf", x_all, d_proj, preferred_element_type=jnp.float32)
        d_proj_here = lax.all_to_all(d_proj, "narrow", split_axis=2, concat_axis=3, tiled=True)
        grad_parts.append(
            d_first
            + jnp.einsum(
                "crsf,dcf->rsd", d_proj_here, whole_qkv, preferred_element_type=jnp.float32
            )
        )
        grad_set = (grad_qkv, grad_out, grad_up, grad_down)
        shares = reduce_grads(grad_set)
        grad_shares = (
            shares
            if grad_shares is None
            else tuple((left + right for left, right in zip(grad_shares, shares)))
        )
    placed_query = lax.dynamic_update_slice_in_dim(
        zero_width, sum_query_bias, narrow_index * local_width, 0
    )
    placed_value = lax.dynamic_update_slice_in_dim(
        zero_width, sum_value_bias, narrow_index * local_width, 0
    )
    placed_up = lax.dynamic_update_slice_in_dim(
        jnp.zeros(up_bias_all.shape, jnp.float32), sum_up_bias, narrow_index * local_hidden, 0
    )
    bias_terms = jnp.stack(
        [placed_query, placed_value, sum_out_bias, sum_down_bias, sum_shift_one, sum_shift_two]
    )
    gain_terms = jnp.stack([sum_gain_one, sum_gain_two])
    grad_b_up, grad_biases, grad_gains = (
        lax.psum_scatter(placed_up, ("wide", "narrow"), scatter_dimension=0, tiled=True),
        lax.psum_scatter(bias_terms, ("wide", "narrow"), scatter_dimension=1, tiled=True),
        lax.psum_scatter(gain_terms, ("wide", "narrow"), scatter_dimension=1, tiled=True),
    )
    output = jnp.concatenate(output_parts, 0)
    grad_tokens = jnp.concatenate(grad_parts, 0)
    return (
        output,
        grad_tokens,
        grad_shares[0],
        grad_shares[1],
        grad_shares[2],
        grad_shares[3],
        grad_b_up,
        grad_biases,
        grad_gains,
    )


def trade_halves(piece, even):
    own = jnp.where(even, piece[0], piece[1])
    give = jnp.where(even, piece[1], piece[0])
    got = lax.ppermute(give, "narrow", PAIRS)
    first = jnp.where(even, own, got)
    second = jnp.where(even, got, own)
    return jnp.concatenate([first, second], 0)


def return_halves(item, even):
    half = item.shape[0] // 2
    own = jnp.where(even, item[:half], item[half:])
    give = jnp.where(even, item[half:], item[:half])
    got = lax.ppermute(give, "narrow", PAIRS)
    return jnp.stack([jnp.where(even, own, got), jnp.where(even, got, own)])


def gather_all(shard):
    return lax.all_gather(shard, ("wide", "narrow"), axis=0, tiled=False)


def scatter_all(blocks):
    return lax.psum_scatter(
        blocks.astype(jnp.bfloat16), ("wide", "narrow"), scatter_dimension=0, tiled=False
    ).astype(jnp.float32)


def mm(spec, left, right):
    return jnp.einsum(spec, left, right, preferred_element_type=jnp.float32)


def item_shards(
    tokens, timestep, context, w_qkv, w_out, w_up, w_down, b_up, biases, gains, cotangent
):
    wide = lax.axis_size("wide")
    narrow = lax.axis_size("narrow")
    z = lax.axis_index("narrow")
    even = z % 2 == 0
    width = tokens.shape[2]
    heads = width // HEAD_DIM
    bias_all, gain_all, up_bias = (
        lax.all_gather(biases, ("wide", "narrow"), axis=1, tiled=True).astype(jnp.float32),
        lax.all_gather(gains, ("wide", "narrow"), axis=1, tiled=True).astype(jnp.float32),
        lax.all_gather(b_up, ("wide", "narrow"), axis=0, tiled=True).astype(jnp.float32),
    )
    token_item = trade_halves(tokens, even).astype(jnp.float32)
    cot = trade_halves(cotangent, even).astype(jnp.float32)
    row = z % 2
    embed = jnp.where(even, timestep[0], timestep[1]).astype(jnp.float32)
    start = context[row, z // 2]
    offset = jnp.arange(ITEM, dtype=jnp.int32)
    noisy = (offset >= start) & (offset < start + NOISE)
    valid = offset[:KEYS] < start + NOISE
    x = token_item + jnp.where(noisy[:, None], embed[None], 0.0)
    xr = x.astype(jnp.bfloat16)

    all_qkv = gather_all(w_qkv.transpose(1, 0, 2))
    all_out = gather_all(w_out)
    all_up = gather_all(w_up)
    all_down = gather_all(w_down)
    wq = all_qkv.reshape(wide, narrow, 3, -1, w_qkv.shape[2])
    wq = wq.transpose(2, 0, 3, 1, 4).reshape(3, width, width)
    wo = all_out.reshape((wide, narrow) + w_out.shape).transpose(1, 2, 0, 3).reshape(width, width)
    wu = all_up.reshape((wide, narrow) + w_up.shape).transpose(0, 2, 1, 3).reshape(width, -1)
    wd = all_down.reshape((wide, narrow) + w_down.shape).transpose(1, 2, 0, 3).reshape(-1, width)

    q = (mm("sd,df->sf", xr, wq[0]) + bias_all[0]).astype(jnp.bfloat16)
    k = mm("sd,df->sf", xr[:KEYS], wq[1]).astype(jnp.bfloat16)
    v = (mm("sd,df->sf", xr[:KEYS], wq[2]) + bias_all[1]).astype(jnp.bfloat16)
    q = q.reshape(ITEM, heads, HEAD_DIM)
    k = k.reshape(KEYS, heads, HEAD_DIM)
    v = v.reshape(KEYS, heads, HEAD_DIM)
    scale = HEAD_DIM**-0.5
    scores = jnp.where(valid, mm("qhe,khe->hqk", q, k) * scale, -jnp.inf)
    probs = jax.nn.softmax(scores, axis=-1)
    low = probs.astype(jnp.bfloat16)
    attended = mm("hqk,khe->qhe", low, v).reshape(ITEM, width).astype(jnp.bfloat16)
    h1 = x + mm("sf,fd->sd", attended, wo) + bias_all[2]
    y1, n1, s1 = norm_forward(h1, gain_all[0], bias_all[4])
    y1r = y1.astype(jnp.bfloat16)
    pre = mm("sd,df->sf", y1r, wu) + up_bias
    act, pull = jax.vjp(partial(jax.nn.gelu, approximate=False), pre)
    act = act.astype(jnp.bfloat16)
    h2 = y1 + mm("sf,fd->sd", act, wd) + bias_all[3]
    result, n2, s2 = norm_forward(h2, gain_all[1], bias_all[5])
    output = return_halves(result.astype(jnp.bfloat16), even)

    dh2 = norm_backward(cot, n2, s2, gain_all[1])
    dh2r = dh2.astype(jnp.bfloat16)
    d_pre = pull(mm("sd,fd->sf", dh2r, wd))[0]
    d_prer = d_pre.astype(jnp.bfloat16)
    g_down = mm("sf,sd->fd", act, dh2r)
    g_down = g_down.reshape((narrow, w_down.shape[0], wide, -1)).transpose(2, 0, 1, 3)
    g_down = scatter_all(g_down.reshape((wide * narrow,) + w_down.shape))
    g_up = mm("sd,sf->df", y1r, d_prer)
    g_up = g_up.reshape((wide, w_up.shape[0], narrow, -1)).transpose(0, 2, 1, 3)
    g_up = scatter_all(g_up.reshape((wide * narrow,) + w_up.shape))
    dy1 = dh2 + mm("sf,df->sd", d_prer, wu)
    dh1 = norm_backward(dy1, n1, s1, gain_all[0])
    dh1r = dh1.astype(jnp.bfloat16)
    g_out = mm("sf,sd->fd", attended, dh1r)
    g_out = g_out.reshape((narrow, w_out.shape[0], wide, -1)).transpose(2, 0, 1, 3)
    g_out = scatter_all(g_out.reshape((wide * narrow,) + w_out.shape))
    d_att = mm("sd,fd->sf", dh1r, wo).astype(jnp.bfloat16).reshape(ITEM, heads, HEAD_DIM)
    d_prob = mm("qhe,khe->hqk", d_att, v)
    d_score = probs * (d_prob - jnp.sum(probs * d_prob, -1, keepdims=True))
    d_score = d_score.astype(jnp.bfloat16)
    d_q = (mm("hqk,khe->qhe", d_score, k) * scale).reshape(ITEM, width)
    d_k = (mm("hqk,qhe->khe", d_score, q) * scale).reshape(KEYS, width)
    d_v = mm("hqk,qhe->khe", low, d_att).reshape(KEYS, width)
    dq, dk, dv = (d_q.astype(jnp.bfloat16), d_k.astype(jnp.bfloat16), d_v.astype(jnp.bfloat16))
    g_qkv = jnp.stack(
        [
            mm("sd,sf->df", xr, dq),
            mm("sd,sf->df", xr[:KEYS], dk),
            mm("sd,sf->df", xr[:KEYS], dv),
        ]
    )
    g_qkv = g_qkv.reshape(3, wide, -1, narrow, w_qkv.shape[2]).transpose(1, 3, 0, 2, 4)
    g_qkv = scatter_all(g_qkv.reshape((wide * narrow, 3) + g_qkv.shape[3:])).transpose(1, 0, 2)
    d_x = dh1 + mm("sf,df->sd", dq, wq[0])
    d_keys_x = mm("sf,df->sd", dk, wq[1]) + mm("sf,df->sd", dv, wq[2])
    d_x = d_x + jnp.pad(d_keys_x, ((0, ITEM - KEYS), (0, 0)))
    grad_tokens = return_halves(d_x.astype(jnp.bfloat16), even).astype(jnp.float32)

    bias_terms = jnp.stack(
        [
            jnp.sum(d_q, 0),
            jnp.sum(d_v, 0),
            jnp.sum(dh1, 0),
            jnp.sum(dh2, 0),
            jnp.sum(dy1, 0),
            jnp.sum(cot, 0),
        ]
    )
    gain_terms = jnp.stack([jnp.sum(dy1 * n1, 0), jnp.sum(cot * n2, 0)])
    grad_b_up, grad_biases, grad_gains = (
        lax.psum_scatter(
            jnp.sum(d_pre, 0), ("wide", "narrow"), scatter_dimension=0, tiled=True
        ),
        lax.psum_scatter(bias_terms, ("wide", "narrow"), scatter_dimension=1, tiled=True),
        lax.psum_scatter(gain_terms, ("wide", "narrow"), scatter_dimension=1, tiled=True),
    )
    return (output, grad_tokens, g_qkv, g_out, g_up, g_down, grad_b_up, grad_biases, grad_gains)


def solution(mesh):
    placed = (
        P("wide", "narrow", None),
        P("wide", None),
        P("wide", None),
        P("wide", None, "narrow"),
        P("narrow", "wide"),
        P("wide", "narrow"),
        P("narrow", "wide"),
        P(("wide", "narrow")),
        P(None, ("wide", "narrow")),
        P(None, ("wide", "narrow")),
        P("wide", "narrow", None),
    )
    by_item = mesh.shape["narrow"] == 4 and mesh.shape["wide"] == 8
    return jax.shard_map(
        item_shards if by_item else shards,
        mesh=mesh,
        in_specs=placed,
        out_specs=(
            P("wide", "narrow", None),
            P("wide", "narrow", None),
            P("wide", None, "narrow"),
            P("narrow", "wide"),
            P("wide", "narrow"),
            P("narrow", "wide"),
            P(("wide", "narrow")),
            P(None, ("wide", "narrow")),
            P(None, ("wide", "narrow")),
        ),
        check_vma=False,
    )
```

```python
from functools import partial

import jax
import jax.numpy as jnp
from jax import lax
from jax.experimental import pallas as pl
from jax.experimental.pallas import tpu as pltpu
from jax.sharding import PartitionSpec as P

HEAD_DIM = 64
ITEM = 592
NOISE = 25
MB = 2
KEYS = 512
PAIRS = ((0, 1), (1, 0), (2, 3), (3, 2))


def spread_rows(piece):
    return lax.all_gather(piece, "narrow", axis=1, tiled=True)


def collect_sums(term):
    return lax.psum_scatter(
        term.astype(jnp.bfloat16), "narrow", scatter_dimension=1, tiled=True
    ).astype(jnp.float32)


def fetch_weights(w_qkv, w_out, w_up, w_down):
    full_qkv, full_out, full_up, full_down = (
        lax.all_gather(w_qkv, "wide", axis=0, tiled=True),
        lax.all_gather(w_out, "wide", axis=1, tiled=True),
        lax.all_gather(w_up, "wide", axis=0, tiled=True),
        lax.all_gather(w_down, "wide", axis=1, tiled=True),
    )
    whole_qkv, whole_out = (
        lax.all_gather(full_qkv, "narrow", axis=2, tiled=True),
        lax.all_gather(full_out, "narrow", axis=0, tiled=True),
    )
    return (whole_qkv, whole_out, full_up, full_down)


def reduce_grads(grad_set):
    return (
        lax.psum_scatter(
            grad_set[0].astype(jnp.bfloat16), "wide", scatter_dimension=0, tiled=True
        ).astype(jnp.float32),
        lax.psum_scatter(
            grad_set[1].astype(jnp.bfloat16), "wide", scatter_dimension=1, tiled=True
        ).astype(jnp.float32),
        lax.psum_scatter(
            grad_set[2].astype(jnp.bfloat16), "wide", scatter_dimension=0, tiled=True
        ).astype(jnp.float32),
        lax.psum_scatter(
            grad_set[3].astype(jnp.bfloat16), "wide", scatter_dimension=1, tiled=True
        ).astype(jnp.float32),
    )


def norm_forward(hidden, gain_vec, shift_vec):
    center = hidden - jnp.mean(hidden, -1, keepdims=True)
    inverse = lax.rsqrt(jnp.mean(center * center, -1, keepdims=True) + 1e-05)
    normed = center * inverse
    return (normed * gain_vec + shift_vec, normed, inverse)


def norm_backward(upstream, normed, inverse, gain_vec):
    scaled = upstream * gain_vec
    return inverse * (
        scaled
        - jnp.mean(scaled, -1, keepdims=True)
        - normed * jnp.mean(scaled * normed, -1, keepdims=True)
    )


def masked_scores(queries, key_rows, key_valid):
    scores = jnp.einsum("qhe,khe->hqk", queries, key_rows, preferred_element_type=jnp.float32)
    scores = scores * queries.shape[-1] ** (-0.5)
    item_index = jnp.arange(queries.shape[0], dtype=jnp.int32) // ITEM
    allowed = (item_index[:, None] == item_index[None, :]) & key_valid[None, :]
    return jnp.where(allowed[None, :, :], scores, -jnp.inf)


def attend_row(inputs):
    queries, key_rows, value_rows, key_valid = inputs
    scores = masked_scores(queries, key_rows, key_valid)
    top_score = jnp.max(scores, -1, keepdims=True)
    log_total = top_score + jnp.log(jnp.sum(jnp.exp(scores - top_score), -1, keepdims=True))
    probs_low = jnp.exp(scores - log_total).astype(jnp.bfloat16)
    attended = jnp.einsum("hqk,khe->qhe", probs_low, value_rows, preferred_element_type=jnp.float32)
    return (attended.reshape(attended.shape[0], -1).astype(jnp.bfloat16), log_total)


def attend_back(inputs):
    queries, key_rows, value_rows, key_valid, log_total, d_att = inputs
    probs = jnp.exp(masked_scores(queries, key_rows, key_valid) - log_total)
    probs_low = probs.astype(jnp.bfloat16)
    d_prob = jnp.einsum("qhe,khe->hqk", d_att, value_rows, preferred_element_type=jnp.float32)
    d_score = probs * (d_prob - jnp.sum(probs * d_prob, -1, keepdims=True))
    d_score_low = d_score.astype(jnp.bfloat16)
    factor = queries.shape[-1] ** (-0.5)
    d_queries = (
        jnp.einsum("hqk,khe->qhe", d_score_low, key_rows, preferred_element_type=jnp.float32)
        * factor
    )
    d_keys = (
        jnp.einsum("hqk,qhe->khe", d_score_low, queries, preferred_element_type=jnp.float32)
        * factor
    )
    d_values = jnp.einsum("hqk,qhe->khe", probs_low, d_att, preferred_element_type=jnp.float32)
    return (d_queries, d_keys, d_values)


def shards(tokens, timestep, context, w_qkv, w_out, w_up, w_down, b_up, biases, gains, cotangent):
    narrow_count = lax.axis_size("narrow")
    narrow_index = lax.axis_index("narrow")
    rows_here, piece_len, model_width = tokens.shape
    seq_len = piece_len * narrow_count
    local_width = w_qkv.shape[2]
    local_hidden = w_up.shape[1]
    heads_here = local_width // HEAD_DIM
    batch_rows = rows_here // MB
    bias_all, gain_all, up_bias_all = (
        lax.all_gather(biases, ("wide", "narrow"), axis=1, tiled=True),
        lax.all_gather(gains, ("wide", "narrow"), axis=1, tiled=True),
        lax.all_gather(b_up, ("wide", "narrow"), axis=0, tiled=True),
    )
    bias_all = bias_all.astype(jnp.float32)
    gain_all = gain_all.astype(jnp.float32)
    up_bias_all = up_bias_all.astype(jnp.float32)
    query_bias = lax.dynamic_slice_in_dim(bias_all[0], narrow_index * local_width, local_width)
    value_bias = lax.dynamic_slice_in_dim(bias_all[1], narrow_index * local_width, local_width)
    up_bias = lax.dynamic_slice_in_dim(up_bias_all, narrow_index * local_hidden, local_hidden)
    position = jnp.arange(seq_len, dtype=jnp.int32)
    item_index = position // ITEM
    offset = position - item_index * ITEM
    item_start = jnp.where(item_index[None, :] == 0, context[:, 0:1], context[:, 1:2])
    noisy_mask = (offset[None, :] >= item_start) & (offset[None, :] < item_start + NOISE)
    key_valid = offset[None, :] < item_start + NOISE
    noisy_here = lax.dynamic_slice_in_dim(noisy_mask, narrow_index * piece_len, piece_len, 1)
    grad_shares = None
    zero_width = jnp.zeros((model_width,), jnp.float32)
    sum_query_bias = jnp.zeros((local_width,), jnp.float32)
    sum_value_bias = jnp.zeros((local_width,), jnp.float32)
    sum_up_bias = jnp.zeros(up_bias.shape, jnp.float32)
    sum_out_bias = zero_width
    sum_down_bias = zero_width
    sum_shift_one = zero_width
    sum_shift_two = zero_width
    sum_gain_one = zero_width
    sum_gain_two = zero_width
    output_parts = []
    grad_parts = []
    head_shape = (batch_rows, seq_len, heads_here, HEAD_DIM)
    for batch in range(MB):
        row_range = slice(batch * batch_rows, (batch + 1) * batch_rows)
        token_part = tokens[row_range].astype(jnp.float32)
        embed_part = timestep[row_range].astype(jnp.float32)
        valid_part = key_valid[row_range]
        x_here = token_part + jnp.where(
            noisy_here[row_range][:, :, None], embed_part[:, None, :], 0.0
        )
        whole_qkv, whole_out, full_up, full_down = fetch_weights(w_qkv, w_out, w_up, w_down)
        local_qkv = lax.dynamic_slice_in_dim(whole_qkv, narrow_index * local_width, local_width, 2)
        local_out = lax.dynamic_slice_in_dim(whole_out, narrow_index * local_width, local_width, 0)
        x_all = spread_rows(x_here.astype(jnp.bfloat16))
        projected = jnp.einsum(
            "rsd,dcf->crsf", x_all, local_qkv, preferred_element_type=jnp.float32
        )
        queries = (projected[0] + query_bias).astype(jnp.bfloat16).reshape(head_shape)
        key_rows = projected[1].astype(jnp.bfloat16).reshape(head_shape)
        value_rows = (projected[2] + value_bias).astype(jnp.bfloat16).reshape(head_shape)
        attended, log_total = lax.map(attend_row, (queries, key_rows, value_rows, valid_part))
        attended_here = lax.all_to_all(attended, "narrow", split_axis=1, concat_axis=2, tiled=True)
        first_sum = (
            x_here
            + jnp.einsum(
                "rsf,fd->rsd", attended_here, whole_out, preferred_element_type=jnp.float32
            )
            + bias_all[2]
        )
        first_norm, normed_one, inverse_one = norm_forward(first_sum, gain_all[0], bias_all[4])
        ffn_input = spread_rows(first_norm.astype(jnp.bfloat16))
        pre_act = (
            jnp.einsum("rsd,df->rsf", ffn_input, full_up, preferred_element_type=jnp.float32)
            + up_bias
        )
        activated, gelu_pull = jax.vjp(partial(jax.nn.gelu, approximate=False), pre_act)
        activated = activated.astype(jnp.bfloat16)
        down_term = jnp.einsum(
            "rsf,fd->rsd", activated, full_down, preferred_element_type=jnp.float32
        )
        second_sum = first_norm + collect_sums(down_term) + bias_all[3]
        result, normed_two, inverse_two = norm_forward(second_sum, gain_all[1], bias_all[5])
        output_parts.append(result.astype(jnp.bfloat16))
        cot_part = cotangent[row_range].astype(jnp.float32)
        sum_gain_two = sum_gain_two + jnp.sum(cot_part * normed_two, (0, 1))
        sum_shift_two = sum_shift_two + jnp.sum(cot_part, (0, 1))
        d_second = norm_backward(cot_part, normed_two, inverse_two, gain_all[1])
        sum_down_bias = sum_down_bias + jnp.sum(d_second, (0, 1))
        d_second_all = spread_rows(d_second.astype(jnp.bfloat16))
        grad_down = jnp.einsum(
            "rsf,rsd->fd", activated, d_second_all, preferred_element_type=jnp.float32
        )
        d_act = jnp.einsum(
            "rsd,fd->rsf", d_second_all, full_down, preferred_element_type=jnp.float32
        )
        d_pre = gelu_pull(d_act)[0]
        sum_up_bias = sum_up_bias + jnp.sum(d_pre, (0, 1))
        d_pre_low = d_pre.astype(jnp.bfloat16)
        grad_up = jnp.einsum(
            "rsd,rsf->df", ffn_input, d_pre_low, preferred_element_type=jnp.float32
        )
        back_term = jnp.einsum(
            "rsf,df->rsd", d_pre_low, full_up, preferred_element_type=jnp.float32
        )
        d_first_norm = d_second + collect_sums(back_term)
        sum_gain_one = sum_gain_one + jnp.sum(d_first_norm * normed_one, (0, 1))
        sum_shift_one = sum_shift_one + jnp.sum(d_first_norm, (0, 1))
        d_first = norm_backward(d_first_norm, normed_one, inverse_one, gain_all[0])
        sum_out_bias = sum_out_bias + jnp.sum(d_first, (0, 1))
        d_first_all = spread_rows(d_first.astype(jnp.bfloat16))
        grad_out = jnp.einsum(
            "rsf,rsd->fd", attended, d_first_all, preferred_element_type=jnp.float32
        )
        d_att = jnp.einsum(
            "rsd,fd->rsf", d_first_all, local_out, preferred_element_type=jnp.float32
        ).astype(jnp.bfloat16)
        d_queries, d_keys, d_values = lax.map(
            attend_back,
            (queries, key_rows, value_rows, valid_part, log_total, d_att.reshape(head_shape)),
        )
        flat_shape = (batch_rows, seq_len, local_width)
        d_queries = d_queries.reshape(flat_shape)
        d_keys = d_keys.reshape(flat_shape)
        d_values = d_values.reshape(flat_shape)
        sum_query_bias = sum_query_bias + jnp.sum(d_queries, (0, 1))
        sum_value_bias = sum_value_bias + jnp.sum(d_values, (0, 1))
        d_proj = jnp.stack([d_queries, d_keys, d_values]).astype(jnp.bfloat16)
        grad_qkv = jnp.einsum("rsd,crsf->dcf", x_all, d_proj, preferred_element_type=jnp.float32)
        d_proj_here = lax.all_to_all(d_proj, "narrow", split_axis=2, concat_axis=3, tiled=True)
        grad_parts.append(
            d_first
            + jnp.einsum(
                "crsf,dcf->rsd", d_proj_here, whole_qkv, preferred_element_type=jnp.float32
            )
        )
        grad_set = (grad_qkv, grad_out, grad_up, grad_down)
        shares = reduce_grads(grad_set)
        grad_shares = (
            shares
            if grad_shares is None
            else tuple((left + right for left, right in zip(grad_shares, shares)))
        )
    placed_query = lax.dynamic_update_slice_in_dim(
        zero_width, sum_query_bias, narrow_index * local_width, 0
    )
    placed_value = lax.dynamic_update_slice_in_dim(
        zero_width, sum_value_bias, narrow_index * local_width, 0
    )
    placed_up = lax.dynamic_update_slice_in_dim(
        jnp.zeros(up_bias_all.shape, jnp.float32), sum_up_bias, narrow_index * local_hidden, 0
    )
    bias_terms = jnp.stack(
        [placed_query, placed_value, sum_out_bias, sum_down_bias, sum_shift_one, sum_shift_two]
    )
    gain_terms = jnp.stack([sum_gain_one, sum_gain_two])
    grad_b_up, grad_biases, grad_gains = (
        lax.psum_scatter(placed_up, ("wide", "narrow"), scatter_dimension=0, tiled=True),
        lax.psum_scatter(bias_terms, ("wide", "narrow"), scatter_dimension=1, tiled=True),
        lax.psum_scatter(gain_terms, ("wide", "narrow"), scatter_dimension=1, tiled=True),
    )
    output = jnp.concatenate(output_parts, 0)
    grad_tokens = jnp.concatenate(grad_parts, 0)
    return (
        output,
        grad_tokens,
        grad_shares[0],
        grad_shares[1],
        grad_shares[2],
        grad_shares[3],
        grad_b_up,
        grad_biases,
        grad_gains,
    )


FWD_PLAN = (
    ("sxy",),
    ("xy", 2, 0),
    ("xy", 3, 0),
    ("fw", 1, 0),
    ("xy", 1, 1),
    ("xy", 1, 2),
    ("dg", 1, 0),
    ("xy", 1, 3),
    ("fw", 1, 1),
    ("fw", 1, 2),
    ("C", "build"),
    ("fw", 1, 3),
    ("fw", 2, 0),
    ("xy", 2, 1),
    ("xy", 2, 2),
    ("xy", 2, 3),
    ("C", "qkv"),
    ("dg", 1, 1),
    ("dg", 1, 2),
    ("dg", 2, 0),
    ("dg", 1, 3),
    ("sfw",),
    ("fw", 3, 0),
    ("fw", 2, 1),
    ("C", "qkv"),
    ("fw", 2, 2),
    ("C", "qkv"),
    ("fw", 2, 3),
    ("xy", 3, 1),
    ("C", "qkv"),
    ("sz",),
    ("C", "att"),
    ("C", "att"),
    ("xy", 3, 2),
    ("C", "att"),
    ("C", "att"),
    ("dg", 3, 0),
    ("dg", 2, 1),
    ("dg", 2, 2),
    ("dg", 2, 3),
    ("C", "att"),
    ("xy", 3, 3),
    ("C", "att"),
    ("C", "att"),
    ("C", "att"),
    ("fw", 3, 1),
    ("C", "out"),
    ("C", "out"),
    ("C", "out"),
    ("C", "out"),
    ("C", "norm1"),
    ("C", "up"),
    ("fw", 3, 2),
    ("C", "up"),
    ("C", "up"),
    ("C", "up"),
    ("fw", 3, 3),
    ("xy", 4, 0),
    ("xy", 4, 1),
    ("xy", 4, 2),
    ("xy", 4, 3),
    ("dg", 3, 1),
    ("dg", 3, 2),
    ("dg", 3, 3),
    ("C", "up"),
    ("C", "up"),
    ("sin", 1),
    ("fw", 4, 0),
    ("C", "up"),
    ("C", "up"),
    ("C", "up"),
    ("fw", 4, 1),
    ("C", "up"),
    ("C", "up"),
    ("C", "up"),
    ("C", "up"),
    ("fw", 4, 2),
    ("C", "up"),
    ("C", "up"),
    ("C", "up"),
    ("fw", 4, 3),
    ("dg", 4, 0),
    ("C", "down"),
    ("dg", 4, 1),
    ("dg", 4, 2),
    ("sin", 2),
    ("dg", 4, 3),
    ("C", "down"),
    ("C", "down"),
    ("C", "down"),
    ("C", "side"),
    ("C", "side"),
    ("C", "side"),
    ("sin", 3),
    ("C", "side"),
    ("C", "norm2"),
)


b16 = jnp.bfloat16
f32 = jnp.float32
MESH = pl.DeviceIdType.MESH
ANY = pl.BlockSpec(memory_space=pl.ANY)
VM = pl.BlockSpec(memory_space=pltpu.VMEM)
SM = pl.BlockSpec(memory_space=pltpu.SMEM)
NAMES = ("small", "qkv", "out", "up", "down")
SIDE = 5
ROUTES = NAMES + ("side",)
FULL = {
    "small": (8, 4, 16, 128),
    "qkv": (4, 3, 1024, 256),
    "out": (8, 1024, 128),
    "up": (4, 1024, 1024),
    "down": (8, 4, 1024, 128),
}
QROWS = 640
CUT = 640
HALF = ITEM // 2
NEG = -1e30
NT = (((1,), (1,)), ((), ()))
TN = (((0,), (0,)), ((), ()))
NN = (((1,), (0,)), ((), ()))


def dot(left, right, dims=NN):
    return lax.dot_general(left, right, dims, preferred_element_type=f32)


def span(start, size):
    return pl.ds(pl.multiple_of(start, size), size)


def unit(name, ref, wi, z):
    if name == "small":
        return ref.at[wi, z]
    if name == "qkv":
        return ref.at[z, :, span(wi * 128, 128), :]
    if name == "out":
        return ref.at[wi, span(z * 256, 256), :]
    if name == "up":
        return ref.at[z, span(wi * 128, 128), :]
    return ref.at[wi, z, 0:CUT, :] if name == "down" else ref.at[wi, z, CUT:1024, :]


def quad_of(name, ref, core, z):
    if name == "small":
        return ref.at[span(core * 4, 4), z]
    if name == "qkv":
        return ref.at[z, :, span(core * 512, 512), :]
    if name == "out":
        return ref.at[span(core * 4, 4), span(z * 256, 256), :]
    if name == "up":
        return ref.at[z, span(core * 512, 512), :]
    rows = slice(0, CUT) if name == "down" else slice(CUT, 1024)
    return ref.at[span(core * 4, 4), z, rows, :]


def place_of():
    w = lax.axis_index("wide")
    z = lax.axis_index("narrow")
    core = w % 2
    chip = w // 2
    cx = chip + 1 - 2 * (chip % 2)
    cy = (chip + 2) % 4
    cd = (cx + 2) % 4
    return z, core, chip, cx, cy, cd


def meet(devices):
    bar = pltpu.get_barrier_semaphore()
    for dev in devices:
        pl.semaphore_signal(bar, inc=1, device_id=dev, device_id_type=MESH)
    pl.semaphore_wait(bar, len(devices))


class Links:
    def __init__(self):
        self.z, self.core, self.chip, self.cx, self.cy, self.cd = place_of()
        self.X = {"wide": self.cx * 2 + self.core}
        self.Y = {"wide": self.cy * 2 + self.core}
        self.C = {"wide": self.chip * 2 + 1 - self.core}
        self.sent = []

    def zdev(self, k):
        return {"narrow": (self.z + k) % 4}

    def mate(self):
        return {"narrow": self.z + 1 - 2 * (self.z % 2)}

    def everyone(self):
        return [self.X, self.Y, self.C] + [self.zdev(k) for k in (1, 2, 3)]

    def start(self, make):
        def build():
            src, dst, ssem, rsem, dev = make()
            return pltpu.make_async_remote_copy(
                src_ref=src,
                dst_ref=dst,
                send_sem=ssem,
                recv_sem=rsem,
                device_id=dev,
                device_id_type=MESH,
            )

        build().start()
        self.sent.append(build)

    def got(self, ref, sems, index):
        pltpu.make_async_remote_copy(
            src_ref=ref,
            dst_ref=ref,
            send_sem=sems[0].at[index],
            recv_sem=sems[1].at[index],
            device_id=self.C,
            device_id_type=MESH,
        ).wait_recv()

    def drain(self):
        for build in self.sent:
            build().wait_send()


class Gather(Links):
    def __init__(self, full, sems):
        super().__init__()
        self.full = full
        self.sz, self.sx, self.sy, self.sd, self.sp = (sems[2 * i : 2 * i + 2] for i in range(5))
        self.me = self.core * 4 + self.chip
        self.wx = self.core * 4 + self.cx
        self.wy = self.core * 4 + self.cy
        self.wd = self.core * 4 + self.cd

    def u(self, n, wi, k):
        return unit(ROUTES[n], self.full[min(n, 4)], wi, (self.z + 4 - k) % 4)

    def quad(self, n, core, k):
        return quad_of(ROUTES[n], self.full[min(n, 4)], core, (self.z + 4 - k) % 4)

    def push(self, view, sems, index, dev):
        self.start(lambda: (view(), view(), sems[0].at[index], sems[1].at[index], dev()))

    def z_send(self, n):
        for k in (1, 2, 3):
            self.push(
                lambda: self.u(n, self.me, 0), self.sz, (n, k - 1), lambda k=k: self.zdev(k)
            )

    def xy(self, n, k):
        if k:
            self.got(self.u(n, self.me, k), self.sz, (n, k - 1))
        self.push(lambda: self.u(n, self.me, k), self.sx, (n, k), lambda: self.X)
        self.push(lambda: self.u(n, self.me, k), self.sy, (n, k), lambda: self.Y)

    def fw(self, n, k):
        self.got(self.u(n, self.wx, k), self.sx, (n, k))
        self.got(self.u(n, self.wy, k), self.sy, (n, k))
        if k < 2:
            self.push(lambda: self.u(n, self.wx, k), self.sd, (n, k), lambda: self.Y)
        else:
            self.push(lambda: self.u(n, self.wy, k), self.sd, (n, k), lambda: self.X)

    def share(self, n, k):
        self.push(lambda: self.quad(n, self.core, k), self.sp, (n, k), lambda: self.C)

    def dg(self, n, k):
        self.got(self.u(n, self.wd, k), self.sd, (n, k))
        self.share(n, k)

    def ok(self, n, k):
        self.got(self.quad(n, 1 - self.core, k), self.sp, (n, k))

    def part(self, wi, j):
        rows = (1024 - CUT) // 2
        return self.full[4].at[wi, self.z, CUT + j * rows : CUT + j * rows + rows, :]

    def sxy(self):
        self.push(lambda: self.u(SIDE, self.me, 0), self.sx, (SIDE, 0), lambda: self.X)
        self.push(lambda: self.u(SIDE, self.me, 0), self.sy, (SIDE, 0), lambda: self.Y)

    def sfw(self):
        self.got(self.u(SIDE, self.wx, 0), self.sx, (SIDE, 0))
        self.got(self.u(SIDE, self.wy, 0), self.sy, (SIDE, 0))
        self.push(lambda: self.part(self.wx, 0), self.sd, (SIDE, 0), lambda: self.Y)
        self.push(lambda: self.part(self.wy, 1), self.sd, (SIDE, 1), lambda: self.X)

    def sz_out(self):
        for j in (0, 1):
            self.got(self.part(self.wd, j), self.sd, (SIDE, j))
        for k in (1, 2, 3):
            self.push(
                lambda: self.quad(SIDE, self.core, 0),
                self.sz,
                (SIDE, k - 1),
                lambda k=k: self.zdev(k),
            )
        self.share(SIDE, 0)

    def sin(self, k):
        self.got(self.quad(SIDE, self.core, k), self.sz, (SIDE, k - 1))
        self.share(SIDE, k)


def loop(count, body, events=()):
    def step(i, carry):
        body(i)
        for at, event in enumerate(events):
            if event:
                pl.when(i == at)(lambda event=event: (event(), None)[1])
        return carry

    lax.fori_loop(0, count, step, 0)


def row_loop(body, rows=32):
    whole = ITEM // rows
    loop(whole, lambda i: body(span(i * rows, rows), rows))
    if ITEM % rows:
        body(slice(whole * rows, ITEM), ITEM % rows)


def lanes_of(pair):
    return span(pair * 128, 128)


def head_masks(rows):
    lane = lax.broadcasted_iota(jnp.int32, (rows, 128), 1)
    return lane < 64, lane == 64, lane == 0


def with_bias(own, slot, data, extra):
    return jnp.where(own, data, jnp.where(slot, extra, jnp.zeros_like(data)))


def split_heads(q, k, bias):
    one = jnp.ones((), b16)
    low, at64, at0 = head_masks(q.shape[0])
    qs = q * jnp.asarray(0.125, b16)
    qa = with_bias(low, at64, qs, one)
    qb = with_bias(~low, at0, qs, one)
    low, at64, at0 = head_masks(k.shape[0])
    ka = with_bias(low, at64, k, bias)
    kb = with_bias(~low, at0, k, bias)
    return qa, qb, ka, kb


def attend_pair(q_ref, k_ref, v_ref, kb_ref, att_ref, lse_ref, pair):
    at = lanes_of(pair)
    qa, qb, ka, kb = split_heads(q_ref[:, at], k_ref[:, at], kb_ref[...])
    vt = v_ref[:, at].T
    halves = []
    for j, (qq, kk) in enumerate(((qa, ka), (qb, kb))):
        scores = dot(kk, qq, NT)
        top = jnp.max(scores, axis=0, keepdims=True)
        e = jnp.exp(scores - top)
        total = jnp.sum(e, axis=0, keepdims=True)
        probs = (e * (1.0 / total)).astype(b16)
        lse_ref[2 * pair + j] = top + jnp.log(total)
        halves.append(dot(vt[j * 64 : j * 64 + 64], probs))
    att_ref[:, at] = jnp.concatenate(halves, 0).T.astype(b16)


def fill_bias(ref, begin):
    def body(i):
        slot = i * 16 + lax.broadcasted_iota(jnp.int32, (16, 128), 0)
        ref[span(i * 16, 16), :] = jnp.where(slot < begin + NOISE, 0.0, NEG).astype(b16)

    loop(KEYS // 16, body)


def norm_rows(h):
    center = h - jnp.mean(h, -1, keepdims=True)
    inverse = lax.rsqrt(jnp.mean(center * center, -1, keepdims=True) + 1e-05)
    return center * inverse, inverse


def fold8(values):
    total = values[0:8]
    for i in range(8, values.shape[0], 8):
        total = total + values[i : i + 8]
    return total


FWD_IN = 5 + 2 + 2
SAVED = (
    ("xr", (ITEM, 1024), b16),
    ("q", (QROWS, 1024), b16),
    ("k", (KEYS, 1024), b16),
    ("v", (KEYS, 1024), b16),
    ("att", (QROWS, 1024), b16),
    ("lse", (16, 1, QROWS), f32),
    ("n1", (ITEM, 1024), f32),
    ("s1", (ITEM, 128), f32),
    ("y1r", (ITEM, 1024), b16),
    ("act", (ITEM, 4096), b16),
    ("gp", (ITEM, 4096), b16),
    ("dh2", (ITEM, 1024), f32),
    ("dh2r", (ITEM, 1024), b16),
    ("res", (ITEM, 1024), b16),
    ("bias", (8, 1024), f32),
    ("col", (3, 8, 1024), f32),
)
NS = len(SAVED)


def forward_kernel(*refs):
    shards = refs[:5]
    tokens, cotan, context, embed = refs[5:FWD_IN]
    w_outs = refs[FWD_IN : FWD_IN + 4]
    saves = refs[FWD_IN + 4 : FWD_IN + 4 + NS]
    rest = list(refs[FWD_IN + 4 + NS :])
    full = rest[:5]
    keep = rest[5 : 5 + NS]
    tok, cot, bup, kbias = rest[5 + NS : 9 + NS]
    sems = rest[9 + NS : 19 + NS]
    lsem, xsem, wsem, ssem = rest[19 + NS :]
    xr, q, k, v, att, lse, x, s1, y1r, act, gp, h2, dh2r, res, bias, col = keep
    g = Gather(full, sems)
    spots = [g.u(n, g.me, 0) for n in range(4)] + [full[4].at[g.me, g.z]]
    first = [pltpu.make_async_copy(shards[n], spots[n], lsem.at[n]) for n in range(5)]
    row = g.z % 2
    own = pl.ds(pl.multiple_of(row * HALF, 8), HALF)
    other = pl.ds(pl.multiple_of((1 - row) * HALF, 8), HALF)
    for i, (src, dst) in enumerate(((tokens, tok), (cotan, cot))):
        first.append(pltpu.make_async_copy(src.at[row], dst.at[own], lsem.at[5 + i]))
    for c in first:
        c.start()
    begin = context[row, g.z // 2]
    fill_bias(kbias, begin)
    meet(g.everyone())
    for c in first:
        c.wait()

    def trade(i, src, dst):
        g.start(
            lambda: (src.at[1 - row], dst.at[own], xsem.at[0, i], xsem.at[1, i], g.mate())
        )

    def traded(i, dst):
        g.got(dst.at[other], (xsem.at[0], xsem.at[1]), i)

    g.z_send(0)
    g.z_send(1)
    g.xy(0, 0)
    g.xy(1, 0)
    trade(0, tokens, tok)
    for n in (2, 3):
        g.z_send(n)
    trade(1, cotan, cot)
    g.z_send(4)
    for j in (1, 2, 3):
        g.xy(0, j)
    for j in range(4):
        g.fw(0, j)
    for j in range(4):
        g.dg(0, j)
    q[ITEM:QROWS, :] = jnp.zeros((QROWS - ITEM, 1024), b16)
    lines = jnp.where(row == 0, embed[0:1, :].astype(f32), embed[1:2, :].astype(f32))

    def save(name_index):
        pltpu.make_async_copy(
            keep[name_index], saves[name_index], ssem.at[name_index]
        ).start()

    def save_w(n):
        pltpu.make_async_copy(full[n], w_outs[n - 1], wsem.at[n - 1]).start()

    def build_rows(rows, count):
        slot = rows.start + lax.broadcasted_iota(jnp.int32, (count, 128), 0)
        mask = ((slot >= begin) & (slot < begin + NOISE)).astype(f32)
        for w in range(8):
            wi = (w % 2) * 4 + w // 2
            to = slice(wi * 128, wi * 128 + 128)
            val = tok[rows, w * 128 : w * 128 + 128].astype(f32)
            val = val + mask * lines[:, w * 128 : w * 128 + 128]
            x[rows, to] = val
            xr[rows, to] = val.astype(b16)

    def build(events):
        for event in events[0]:
            event()
        traded(0, tok)
        row_loop(build_rows)
        for k in range(4):
            g.ok(0, k)
        for w in range(8):
            wi = (w % 2) * 4 + w // 2
            total = full[0][wi, 0].astype(f32)
            for zz in (1, 2, 3):
                total = total + full[0][wi, zz].astype(f32)
            bias[:, wi * 128 : wi * 128 + 128] = total[0:8]
            for zz in range(4):
                d = w * 4 + zz
                one = full[0][wi, zz].astype(f32)[8:9]
                bup[d // 8, :, (d % 8) * 128 : (d % 8) * 128 + 128] = one
        for event in events[1]:
            event()

    def project(i):
        zz = (g.z + 4 - i) % 4
        to = span(zz * 256, 256)
        q[0:ITEM, to] = (dot(xr[...], full[1][zz, 0]) + qb_of(bias, 0, zz)).astype(b16)
        k[:, to] = dot(xr[0:KEYS, :], full[1][zz, 1]).astype(b16)
        v[:, to] = (dot(xr[0:KEYS, :], full[1][zz, 2]) + qb_of(bias, 1, zz)).astype(b16)

    def project_out(i):
        to = span(i * 256, 256)
        wo = jnp.concatenate([full[2][2 * i], full[2][2 * i + 1]], 1)
        x[:, to] = x[:, to] + dot(att[0:ITEM, :], wo) + bias[2:3, to]

    def norm_one(rows, count):
        n1, inv = norm_rows(x[rows, :])
        y1 = n1 * bias[6:7, :] + bias[4:5, :]
        x[rows, :] = n1
        s1[rows, :] = jnp.broadcast_to(inv, (count, 128))
        y1r[rows, :] = y1.astype(b16)
        h2[rows, :] = y1 + bias[3:4, :]

    def up(i):
        zz = (g.z + 4 - i // 4) % 4
        cols = span((i % 4) * 256, 256)
        pre = dot(y1r[...], full[3][zz, :, cols]) + bup[zz, :, cols]
        half = 0.5 * (1.0 + lax.erf(pre * 0.7071067811865476))
        slope = half + pre * (jnp.exp(-0.5 * pre * pre) * 0.3989422804014327)
        to = span(zz * 1024 + (i % 4) * 256, 256)
        act[:, to] = (pre * half).astype(b16)
        gp[:, to] = slope.astype(b16)

    def down_rows(lo, hi):
        def body(i):
            zz = (g.z + 4 - i) % 4
            lanes = pl.ds(pl.multiple_of(zz * 1024 + lo, 128), hi - lo)
            hidden = act[:, lanes]
            for j in range(4):
                to = slice(j * 256, j * 256 + 256)
                wd = [full[4][2 * j + e, zz, lo:hi, :] for e in (0, 1)]
                h2[:, to] += dot(hidden, jnp.concatenate(wd, 1))

        return body

    def norm_two(rows, count):
        n2, inv = norm_rows(h2[rows, :])
        out = n2 * bias[7:8, :] + bias[5:6, :]
        parts = []
        for wi in range(8):
            w = (wi % 4) * 2 + wi // 4
            parts.append(cot[rows, w * 128 : w * 128 + 128].astype(f32))
            res[rows, w * 128 : w * 128 + 128] = out[:, wi * 128 : wi * 128 + 128].astype(b16)
        ct = jnp.concatenate(parts, 1)
        e2 = ct * bias[7:8, :]
        grad = inv * (
            e2 - jnp.mean(e2, -1, keepdims=True) - n2 * jnp.mean(e2 * n2, -1, keepdims=True)
        )
        h2[rows, :] = grad
        dh2r[rows, :] = grad.astype(b16)
        col[0] += fold8(ct)
        col[1] += fold8(ct * n2)
        col[2] += fold8(grad)

    def tiles(count, body, needs, after=()):
        def run(events):
            table = [list(group) for group in events]
            for at, need in needs:
                table[at].append(need)
            for event in table[0]:
                event()
            loop(count, body, [group_of(group) for group in table[1:]])
            for item in after:
                item()

        return run

    def saver(indices, weights=()):
        def go():
            for n in weights:
                save_w(n)
            for i in indices:
                save(i)

        return go

    def rows_of(body, before=None, after=None):
        def run(events):
            for event in events[0]:
                event()
            if before:
                before()
            row_loop(body)
            for event in events[1]:
                event()
            if after:
                after()

        return run

    def ready_two():
        traded(1, cot)
        save_w(4)
        col[...] = jnp.zeros_like(col)

    oks = lambda n: [(k, lambda k=k: g.ok(n, k)) for k in range(4)]
    stages = {
        "build": build,
        "qkv": tiles(4, project, oks(1), [saver((0, 14), (1,))]),
        "att": tiles(
            8,
            lambda i: attend_pair(q, k, v, kbias, att, lse, i),
            [],
            [saver((1, 2, 3, 4, 5))],
        ),
        "out": tiles(
            4, project_out, [(0, lambda k=k: g.ok(2, k)) for k in range(4)], [lambda: save_w(2)]
        ),
        "norm1": rows_of(norm_one, None, saver((6, 7, 8))),
        "up": tiles(
            16, up, [(4 * k, lambda k=k: g.ok(3, k)) for k in range(4)], [saver((9, 10), (3,))]
        ),
        "down": tiles(4, down_rows(0, CUT), oks(4)),
        "side": tiles(4, down_rows(CUT, 1024), oks(SIDE)),
        "norm2": rows_of(norm_two, ready_two, saver((11, 12, 13, 15))),
    }
    moves = {
        "xy": g.xy,
        "fw": g.fw,
        "dg": g.dg,
        "sxy": g.sxy,
        "sfw": g.sfw,
        "sz": g.sz_out,
        "sin": g.sin,
    }
    spots = []
    for step in FWD_PLAN:
        if step[0] == "C":
            if not spots or spots[-1][0] != step[1]:
                lead = spots.pop()[1][-1] if spots and spots[-1][0] is None else []
                spots.append((step[1], [lead]))
            spots[-1][1].append([])
            continue
        if not spots:
            spots.append((None, [[]]))
        spots[-1][1][-1].append(lambda step=step: moves[step[0]](*step[1:]))
    for name, events in spots:
        stages[name](events)
    for i in range(NS):
        pltpu.make_async_copy(keep[i], saves[i], ssem.at[i]).wait()
    for n in (1, 2, 3, 4):
        pltpu.make_async_copy(full[n], w_outs[n - 1], wsem.at[n - 1]).wait()
    g.drain()


def group_of(group):
    def go():
        for event in group:
            event()

    return go if group else None


def qb_of(bias, which, i):
    parts = [bias[which : which + 1, span((j * 4 + i) * 128, 128)] for j in (0, 1)]
    return jnp.concatenate(parts, 1)


def forward(shards, tokens, cotan, context, embed):
    dma = pltpu.SemaphoreType.DMA
    scratch = [pltpu.VMEM(FULL[n], b16) for n in NAMES]
    scratch += [pltpu.VMEM(shape, kind) for _, shape, kind in SAVED]
    scratch += [pltpu.VMEM((ITEM, 1024), b16)] * 2 + [pltpu.VMEM((4, 1, 1024), f32)]
    scratch += [pltpu.VMEM((KEYS, 128), b16)]
    scratch += [dma((6, 3))] * 2 + [dma((6, 4))] * 8
    scratch += [dma((7,)), dma((2, 2)), dma((4,)), dma((NS,))]
    shapes = [jax.ShapeDtypeStruct(FULL[n], b16) for n in NAMES[1:]]
    shapes += [jax.ShapeDtypeStruct(shape, kind) for _, shape, kind in SAVED]
    return pl.pallas_call(
        forward_kernel,
        out_shape=shapes,
        in_specs=[ANY] * 7 + [SM, VM],
        out_specs=[ANY] * len(shapes),
        scratch_shapes=scratch,
        compiler_params=pltpu.CompilerParams(
            collective_id=0, has_side_effects=True, vmem_limit_bytes=66000000
        ),
    )(*shards, tokens, cotan, context, embed)


def to_blocks(features):
    parts = features.reshape(features.shape[:-1] + (4, 2, 128))
    return jnp.swapaxes(parts, -3, -2).reshape(features.shape)


def pack_vectors(b_up, biases, gains):
    lane_group = jnp.arange(128, dtype=jnp.int32) // 32
    eight = jnp.concatenate([biases, gains], 0)
    z = lax.axis_index("narrow")
    spread = jnp.where(lane_group == z, jnp.tile(eight, (1, 4)), jnp.zeros((), b16))
    return jnp.concatenate([spread, b_up[None], jnp.zeros((7, 128), b16)], 0)


UNIT = {
    "small": (16, 128),
    "qkv": (3, 128, 256),
    "out": (256, 128),
    "up": (128, 1024),
    "down": (CUT, 128),
    "side": (1024 - CUT, 128),
}
FINAL = dict(UNIT, down=(1024, 128))
ORDER = (1, 2, 3, 0)


def half_of(name, ref, core, z):
    if name == "small":
        return ref.at[span(core * 4, 4), z]
    if name == "qkv":
        return ref.at[z, :, span(core * 512, 512), :]
    if name == "up":
        return ref.at[z, span(core * 512, 512), :]
    if name == "down":
        return ref.at[span(core * 4, 4), z]
    return ref.at[span(core * 4, 4), span(z * 256, 256), :]


def add_into(name, target, sources, count=8):
    rows = UNIT[name][-2] // count

    def step(i):
        at = span(i * rows, rows)
        at = (slice(None), at) if name == "qkv" else at
        total = target[at].astype(f32)
        for source in sources:
            total = total + source[at].astype(f32)
        target[at] = total.astype(target.dtype)

    loop(count, step)


class Scatter(Links):
    def __init__(self, grads, recv, side, final, outs, sems, credit, osem):
        super().__init__()
        self.grads = grads
        self.rd, self.rx, self.ry, self.rz = (recv[5 * i : 5 * i + 5] for i in range(4))
        self.side = side
        self.final = final
        self.outs = outs
        self.sp, self.sd, self.sx, self.sy, self.sz = (sems[2 * i : 2 * i + 2] for i in range(5))
        self.credit = credit
        self.osem = osem

    def zz(self, k):
        return (self.z + k) % 4

    def g(self, n, chip, k):
        return unit(NAMES[n], self.grads[n], self.core * 4 + chip, self.zz(k))

    def half(self, n, core, k):
        return half_of(NAMES[n], self.grads[n], core, self.zz(k))

    def free(self, n):
        pl.semaphore_signal(self.credit.at[n], inc=1, device_id=self.C, device_id_type=MESH)

    def may_send(self, n):
        pl.semaphore_wait(self.credit.at[n], 1)

    def push(self, src, dst, sems, index, dev):
        self.start(lambda: (src(), dst(), sems[0].at[index], sems[1].at[index], dev()))

    def swap(self, n, k):
        there = lambda: self.half(n, 1 - self.core, k)
        self.push(there, there, self.sp, (n, k), lambda: self.C)

    def swapped(self, n, k):
        self.got(self.half(n, self.core, k), self.sp, (n, k))

    def to_x(self, n, k):
        self.push(
            lambda: self.g(n, self.cx, k), lambda: self.rx[n].at[k], self.sx, (n, k), lambda: self.X
        )

    def to_y(self, n, k):
        self.push(
            lambda: self.g(n, self.cy, k), lambda: self.ry[n].at[k], self.sy, (n, k), lambda: self.Y
        )

    def first(self, n, k):
        dev = (lambda: self.X) if k < 2 else (lambda: self.Y)
        self.push(
            lambda: self.g(n, self.cd, k), lambda: self.rd[n].at[k], self.sd, (n, k), dev
        )
        if k < 2:
            self.to_x(n, k)
        else:
            self.to_y(n, k)

    def second(self, n, k):
        self.got(self.rd[n].at[k], self.sd, (n, k))
        chip = self.cy if k < 2 else self.cx
        add_into(NAMES[n], self.g(n, chip, k), [self.rd[n].at[k]])
        if k < 2:
            self.to_y(n, k)
        else:
            self.to_x(n, k)

    def third(self, n, k):
        self.got(self.rx[n].at[k], self.sx, (n, k))
        self.got(self.ry[n].at[k], self.sy, (n, k))
        add_into(NAMES[n], self.g(n, self.chip, k), [self.rx[n].at[k], self.ry[n].at[k]])
        self.push(
            lambda: self.g(n, self.chip, k),
            lambda: self.rz[n].at[k - 1],
            self.sz,
            (n, k - 1),
            lambda: self.zdev(k),
        )

    def last(self, n):
        self.got(self.rx[n].at[0], self.sx, (n, 0))
        self.got(self.ry[n].at[0], self.sy, (n, 0))
        for k in (1, 2, 3):
            self.got(self.rz[n].at[k - 1], self.sz, (n, k - 1))
        own = self.g(n, self.chip, 0)
        parts = [own, self.rx[n].at[0], self.ry[n].at[0]] + [self.rz[n].at[j] for j in range(3)]
        name = NAMES[n]
        count = 1 if name == "small" else 8
        rows = UNIT[name][-2] // count

        def step(i):
            at = span(i * rows, rows)
            at = (slice(None), at) if name == "qkv" else at
            total = parts[0][at].astype(f32)
            for part in parts[1:]:
                total = total + part[at].astype(f32)
            self.final[n][at] = total

        loop(count, step)
        if n < 4:
            self.ship(n)

    def ship(self, n):
        pltpu.make_async_copy(self.final[n], self.outs[n], self.osem.at[n]).start()

    def quad(self, k):
        return self.grads[4].at[span(self.core * 4, 4), self.zz(k), CUT:1024, :]

    def mine(self, chip):
        return self.grads[4].at[self.core * 4 + chip, self.z, CUT:1024, :]

    def part(self, chip, j):
        rows = (1024 - CUT) // 2
        at = slice(CUT + j * rows, CUT + j * rows + rows)
        return self.grads[4].at[self.core * 4 + chip, self.z, at, :]

    def side_z(self, k):
        self.push(
            lambda: self.quad(k),
            lambda: self.side[0].at[k - 1],
            self.sz,
            (SIDE, k - 1),
            lambda: self.zdev(k),
        )

    def side_sum(self):
        for k in (1, 2, 3):
            self.got(self.side[0].at[k - 1], self.sz, (SIDE, k - 1))
        for chip in range(4):
            add_into("side", self.mine(chip), [self.side[0].at[j, chip] for j in range(3)], 4)
        for j, dev in enumerate((lambda: self.X, lambda: self.Y)):
            self.push(
                lambda j=j: self.part(self.cd, j),
                lambda j=j: self.side[1].at[j],
                self.sd,
                (SIDE, j),
                dev,
            )

    def side_xy(self):
        for j, chip in enumerate((self.cy, self.cx)):
            self.got(self.side[1].at[j], self.sd, (SIDE, j))
            target = self.part(chip, j)
            target[...] = (target[...].astype(f32) + self.side[1][j].astype(f32)).astype(b16)
        self.push(
            lambda: self.mine(self.cy),
            lambda: self.side[3],
            self.sy,
            (SIDE, 0),
            lambda: self.Y,
        )
        self.push(
            lambda: self.mine(self.cx),
            lambda: self.side[2],
            self.sx,
            (SIDE, 0),
            lambda: self.X,
        )

    def side_last(self):
        self.got(self.side[2], self.sx, (SIDE, 0))
        self.got(self.side[3], self.sy, (SIDE, 0))
        total = self.mine(self.chip)[...].astype(f32)
        total = total + self.side[2][...].astype(f32) + self.side[3][...].astype(f32)
        self.final[4][CUT:1024, :] = total
        self.ship(4)


def attend_pair_back(q_ref, k_ref, v_ref, d_ref, kb_ref, lse_ref, store, pair):
    at = lanes_of(pair)
    qp = q_ref(at)
    kp = k_ref(at)
    vp = v_ref(at)
    dp = d_ref[:, at]
    qa, qb, ka, kb = split_heads(qp, kp, kb_ref[...])
    low, _, _ = head_masks(QROWS)
    none = jnp.zeros((), b16)
    kt = kp.T
    qs = qp * jnp.asarray(0.125, b16)
    d_k = d_v = None
    d_q = []
    for j, (qq, kk) in enumerate(((qa, ka), (qb, kb))):
        own = low if j == 0 else ~low
        probs = jnp.exp(dot(kk, qq, NT) - lse_ref[2 * pair + j])
        d_own = jnp.where(own, dp, none)
        d_prob = dot(vp, d_own, NT)
        delta = jnp.sum(probs * d_prob, axis=0, keepdims=True)
        d_score = (probs * (d_prob - delta)).astype(b16)
        part_v = dot(probs.astype(b16), d_own)
        part_k = dot(d_score, jnp.where(own, qs, none))
        d_v = part_v if d_v is None else d_v + part_v
        d_k = part_k if d_k is None else d_k + part_k
        d_q.append(dot(kt[j * 64 : j * 64 + 64], d_score))
    d_q = (jnp.concatenate(d_q, 0) * 0.125).T
    store(pair, d_q, d_k, d_v)


LOADED = ("dh2", "dh2r", "gp", "act", "y1r", "n1", "s1", "lse", "bias", "col")
LATE = ("q", "k", "v", "att", "xr")


def backward_kernel(*refs):
    w_in = refs[:4]
    load = dict(zip(LOADED + LATE + ("res",), refs[4:20]))
    context = refs[20]
    out, gtok = refs[21:23]
    outs = refs[23:28]
    rest = list(refs[28:])
    take = lambda count: [rest.pop(0) for _ in range(count)]
    grads = take(5)
    recv = take(20)
    side = take(4)
    final = take(5)
    dh, dhr, gp, act, yr, n1, s1, lse, bias, col = take(10)
    stage, back, vec, ups, qsum, vsum, kbias = take(7)
    sems = take(10)
    credit, wsem, lsem, osem, xsem, tsem, dsem = take(7)
    s = Scatter(grads, recv, side, final, outs, sems, credit, osem)
    row = s.z % 2
    own = pl.ds(pl.multiple_of(row * HALF, 8), HALF)
    other = pl.ds(pl.multiple_of((1 - row) * HALF, 8), HALF)

    def wcopy(n):
        return pltpu.make_async_copy(w_in[n - 1], grads[n], wsem.at[n])

    spots = {
        "dh2": dh,
        "dh2r": dhr,
        "gp": gp.at[0:ITEM],
        "act": act,
        "y1r": yr.at[0:ITEM],
        "n1": n1,
        "s1": s1,
        "lse": lse,
        "bias": bias,
        "col": col,
        "q": gp.at[:, 0:1024],
        "k": gp.at[0:KEYS, 1024:2048],
        "v": gp.at[0:KEYS, 2048:3072],
        "att": gp.at[:, 3072:4096],
        "xr": yr.at[0:ITEM],
    }
    names = LOADED + LATE

    def lcopy(name):
        return pltpu.make_async_copy(load[name], spots[name], lsem.at[names.index(name)])

    def old_down(wi):
        cols = slice(wi * 128, wi * 128 + 128)
        return pltpu.make_async_copy(w_in[3].at[wi], grads[3].at[:, :, cols], dsem.at[wi])

    lcopy("dh2r").start()
    lcopy("act").start()
    for wi in range(8):
        old_down(wi).start()
    for name in ("gp", "dh2", "y1r", "n1", "s1", "lse", "bias", "col"):
        lcopy(name).start()
    wcopy(2).start()
    wcopy(1).start()
    stage_in = pltpu.make_async_copy(load["res"].at[own], stage, tsem.at[0])
    stage_out = pltpu.make_async_copy(stage, out.at[row], tsem.at[1])
    stage_in.start()
    fill_bias(kbias, context[row, s.z // 2])
    meet(s.everyone())
    s.start(lambda: (load["res"].at[other], out.at[row], xsem.at[0, 0], xsem.at[1, 0], s.mate()))
    lcopy("dh2r").wait()
    lcopy("act").wait()

    def put4(ref, core, rows, value, add):
        for p in range(4):
            part = value[:, p * 128 : p * 128 + 128]
            if add:
                part = part + ref[core * 4 + p, rows, :].astype(f32)
            ref[core * 4 + p, rows, :] = part.astype(b16)

    def down_tile(core, add):
        def body(i):
            zz = s.zz((i // 4 + 1) % 4)
            at = span(zz * 1024 + (i % 4) * 256, 256)
            value = dot(act[:, at], dhr[:, span(core * 512, 512)], TN)
            put4(grads[4].at[:, zz], core, span((i % 4) * 256, 256), value, add)

        return body

    def ready(n, k):
        if n == 4 and k:
            s.side_z(k)
        s.first(n, k)

    def both(n, tile_of, per, mid=()):
        other_core = 1 - s.core
        theirs = tile_of(other_core, False)

        def body(i):
            theirs(i)
            for j, k in enumerate(ORDER):
                pl.when(i == per * (j + 1) - 1)(lambda k=k: s.swap(n, k))

        loop(4 * per, body, mid)
        mine = tile_of(s.core, True)

        def body2(i):
            for j, k in enumerate(ORDER):
                pl.when(i == per * j)(lambda k=k: s.swapped(n, k))
            mine(i)
            for j, k in enumerate(ORDER):
                pl.when(i == per * (j + 1) - 1)(lambda k=k: ready(n, k))

        loop(4 * per, body2)

    both(4, down_tile, 4)

    lcopy("gp").wait()
    for wi in range(8):
        old_down(wi).wait()

    def d_pre_tile(i):
        to = span(i * 256, 256)
        wd = grads[3][i // 4, span((i % 4) * 256, 256), :]
        d_pre = dot(dhr[...], wd, NT) * gp[0:ITEM, to].astype(f32)
        total = jnp.sum(d_pre, axis=0, keepdims=True)
        ups[2 * i] = total[:, 0:128]
        ups[2 * i + 1] = total[:, 128:256]
        gp[0:ITEM, to] = d_pre.astype(b16)

    wait_a = [None] * 8 + [lambda: s.second(4, 1), None, None, None, lambda: s.second(4, 2)]
    loop(16, d_pre_tile, wait_a)
    wcopy(3).start()
    stage_in.wait()
    stage_out.start()
    lcopy("dh2").wait()
    s.second(4, 3)
    s.second(4, 0)
    wcopy(3).wait()

    def dy1_tile(i):
        to = span(i * 256, 256)
        total = dh[:, to]
        for zz in range(4):
            total = total + dot(
                gp[0:ITEM, zz * 1024 : zz * 1024 + 1024], grads[3][zz, to, :], NT
            )
        dh[:, to] = total

    loop(4, dy1_tile)
    s.free(3)
    lcopy("y1r").wait()
    s.may_send(3)

    def up_tile(core, add):
        def body(i):
            zz = s.zz((i // 2 + 1) % 4)
            cols = span((i % 2) * 512, 512)
            value = dot(
                yr[0:ITEM, span(core * 512, 512)],
                gp[0:ITEM, span(zz * 1024 + (i % 2) * 512, 512)],
                TN,
            )
            rows = span(core * 512, 512)
            if add:
                value = value + grads[3][zz, rows, cols].astype(f32)
            grads[3][zz, rows, cols] = value.astype(b16)

        return body

    both(3, up_tile, 2)
    for name in ("q", "k", "v", "att"):
        lcopy(name).start()
    for name in ("n1", "s1", "lse", "bias", "col"):
        lcopy(name).wait()
    for r in range(3):
        vec[r * 8 : r * 8 + 8, :] = jnp.zeros((8, 1024), f32)

    def norm_one_back(rows, count):
        dy1 = dh[rows, :]
        n = n1[rows, :]
        e1 = dy1 * bias[6:7, :]
        grad = s1[rows, 0:1] * (
            e1 - jnp.mean(e1, -1, keepdims=True) - n * jnp.mean(e1 * n, -1, keepdims=True)
        )
        dh[rows, :] = grad
        dhr[rows, :] = grad.astype(b16)
        vec[0:8, :] += fold8(grad)
        vec[8:16, :] += fold8(dy1)
        vec[16:24, :] += fold8(dy1 * n)

    row_loop(norm_one_back)
    s.third(4, 1)
    wcopy(2).wait()
    yr[ITEM:QROWS, :] = jnp.zeros((QROWS - ITEM, 1024), b16)

    def d_att_tile(i):
        to = span(i * 256, 256)
        wo = jnp.concatenate([grads[2][wi, to, :] for wi in range(8)], 1)
        yr[0:ITEM, to] = dot(dhr[...], wo, NT).astype(b16)

    loop(4, d_att_tile)
    s.free(2)
    for name in ("q", "k", "v", "att"):
        lcopy(name).wait()
    s.third(4, 2)
    s.third(4, 3)
    s.may_send(2)

    def out_tile(core, add):
        def body(i):
            zz = s.zz((i + 1) % 4)
            at = span(zz * 256, 256)
            value = dot(
                gp[0:ITEM, span(3072 + zz * 256, 256)], dhr[:, span(core * 512, 512)], TN
            )
            put4(grads[2], core, at, value, add)

        return body

    both(2, out_tile, 1)

    def store(pair, d_q, d_k, d_v):
        act[:, span(2048 + pair * 128, 128)] = d_q[0:ITEM].astype(b16)
        act[0:KEYS, span(pair * 128, 128)] = d_k.astype(b16)
        act[0:KEYS, span(1024 + pair * 128, 128)] = d_v.astype(b16)
        qsum[pair] = jnp.sum(d_q, axis=0, keepdims=True)
        vsum[pair] = jnp.sum(d_v, axis=0, keepdims=True)

    def pair_back(i):
        attend_pair_back(
            lambda at: gp[:, span(i * 128, 128)],
            lambda at: gp[0:KEYS, span(1024 + i * 128, 128)],
            lambda at: gp[0:KEYS, span(2048 + i * 128, 128)],
            yr,
            kbias,
            lse,
            store,
            i,
        )

    loop(
        8,
        pair_back,
        [
            lambda: s.second(3, 1),
            lambda: s.second(3, 2),
            None,
            lambda: s.second(3, 3),
            lambda: s.second(3, 0),
            lambda: s.last(4),
            lambda: s.side_sum(),
            lambda: s.third(3, 1),
        ],
    )
    lcopy("xr").start()
    wcopy(1).wait()

    def d_x(i):
        src = span(i * 256, 256)
        for c in range(2):
            rows = slice(c * 512, c * 512 + 512)
            dh[:, rows] += dot(act[:, span(2048 + i * 256, 256)], grads[1][i, 0, rows, :], NT)
            keys = dot(act[0:KEYS, src], grads[1][i, 1, rows, :], NT)
            keys = keys + dot(
                act[0:KEYS, span(1024 + i * 256, 256)], grads[1][i, 2, rows, :], NT
            )
            dh[0:KEYS, rows] += keys

    loop(4, d_x)
    s.free(1)
    lcopy("xr").wait()
    s.may_send(1)

    def qkv_tile(core, add):
        def body(i):
            zz = s.zz((i + 1) % 4)
            cols = span(core * 512, 512)
            rows = span(core * 512, 512)
            for c3, (start, height) in enumerate(((2048, ITEM), (0, KEYS), (1024, KEYS))):
                value = dot(
                    yr[0:height, cols], act[0:height, span(start + zz * 256, 256)], TN
                )
                if add:
                    value = value + grads[1][zz, c3, rows, :].astype(f32)
                grads[1][zz, c3, rows, :] = value.astype(b16)

        return body

    both(1, qkv_tile, 1)

    for r in range(3):
        col[r, 0:1, :] = jnp.sum(col[r], axis=0, keepdims=True)
    sums = [jnp.sum(vec[r * 8 : r * 8 + 8, :], axis=0, keepdims=True) for r in range(3)]
    for w in range(8):
        wi = (w % 2) * 4 + w // 2
        vec[0:1, wi * 128 : wi * 128 + 128] = qsum[w]
        vec[1:2, wi * 128 : wi * 128 + 128] = vsum[w]
    vec[2:3, :] = sums[0]
    vec[3:4, :] = col[2, 0:1, :]
    vec[4:5, :] = sums[1]
    vec[5:6, :] = col[0, 0:1, :]
    vec[6:7, :] = sums[2]
    vec[7:8, :] = col[1, 0:1, :]

    def vectors(core, add):
        for p in range(4):
            wi = core * 4 + p
            eight = vec[0:8, span(wi * 128, 128)]
            for zz in range(4):
                one = ups[(p * 2 + core) * 4 + zz]
                value = jnp.concatenate([eight, jnp.broadcast_to(one, (8, 128))], 0)
                if add:
                    value = value + grads[0][wi, zz]
                grads[0][wi, zz] = value

    vectors(1 - s.core, False)
    for k in ORDER:
        s.swap(0, k)

    def ship(i):
        rows = pl.ds(pl.multiple_of((1 - row) * HALF + i * 8, 8), 8)
        for w in range(8):
            wi = (w % 2) * 4 + w // 2
            back[1, pl.ds(pl.multiple_of(i * 8, 8), 8), w * 128 : w * 128 + 128] = dh[
                rows, wi * 128 : wi * 128 + 128
            ].astype(b16)

    loop(HALF // 8, ship)
    s.start(lambda: (back.at[1], back.at[0], xsem.at[0, 1], xsem.at[1, 1], s.mate()))
    mine = []
    for w in range(8):
        wi = (w % 2) * 4 + w // 2
        mine.append(
            pltpu.make_async_copy(
                dh.at[own, wi * 128 : wi * 128 + 128],
                gtok.at[row, :, w * 128 : w * 128 + 128],
                tsem.at[2 + w],
            )
        )
    for c in mine:
        c.start()
    for k in ORDER:
        s.swapped(0, k)
    vectors(s.core, True)
    for k in ORDER:
        s.first(0, k)
    s.third(3, 2)
    for k in ORDER:
        s.second(2, k)
    s.side_xy()
    s.third(3, 3)
    for k in ORDER:
        s.second(0, k)
        s.second(1, k)
    for k in (1, 2, 3):
        s.third(2, k)
    s.last(3)
    s.side_last()
    for k in (1, 2, 3):
        s.third(0, k)
        s.third(1, k)
    s.got(back.at[0], (xsem.at[0], xsem.at[1]), 1)

    def widen(i):
        at = pl.ds(pl.multiple_of(i * 8, 8), 8)
        rows = pl.ds(pl.multiple_of((1 - row) * HALF + i * 8, 8), 8)
        dh[rows, :] = back[0, at, :].astype(f32)

    loop(HALF // 8, widen)
    theirs = pltpu.make_async_copy(dh.at[other], gtok.at[1 - row], tsem.at[10])
    theirs.start()
    s.last(2)
    s.last(0)
    s.last(1)
    for c in mine:
        c.wait()
    theirs.wait()
    stage_out.wait()
    s.got(out.at[1 - row], (xsem.at[0], xsem.at[1]), 0)
    for n in range(5):
        pltpu.make_async_copy(final[n], outs[n], osem.at[n]).wait()
    s.drain()


def backward(weights, saved, context):
    dma = pltpu.SemaphoreType.DMA
    vmem = pltpu.VMEM
    kinds = dict((name, kind) for name, _, kind in SAVED)
    shapes = dict((name, shape) for name, shape, _ in SAVED)
    deep = [f32] + [b16] * 4
    scratch = [vmem(FULL[n], deep[i]) for i, n in enumerate(NAMES)]
    for depth in (4, 4, 4, 3):
        scratch += [vmem((depth,) + UNIT[n], deep[i]) for i, n in enumerate(NAMES)]
    width = 1024 - CUT
    scratch += [vmem((3, 4, width, 128), b16), vmem((2, width // 2, 128), b16)]
    scratch += [vmem((width, 128), b16)] * 2
    scratch += [vmem(FINAL[n], f32) for n in NAMES]
    tall = {"gp": (QROWS, 4096), "y1r": (QROWS, 1024)}
    scratch += [vmem(tall.get(n, shapes[n]), kinds[n]) for n in LOADED]
    scratch += [vmem((HALF, 1024), b16), vmem((2, HALF, 1024), b16), vmem((24, 1024), f32)]
    scratch += [vmem((32, 1, 128), f32), vmem((8, 1, 128), f32), vmem((8, 1, 128), f32)]
    scratch += [vmem((KEYS, 128), b16)]
    scratch += [dma((6, 4))] * 10
    scratch += [pltpu.SemaphoreType.REGULAR((5,)), dma((5,)), dma((15,)), dma((5,))]
    scratch += [dma((2, 2)), dma((11,)), dma((8,))]
    out_shapes = [
        jax.ShapeDtypeStruct((2, HALF, 1024), b16),
        jax.ShapeDtypeStruct((2, HALF, 1024), f32),
    ]
    out_shapes += [jax.ShapeDtypeStruct(FINAL[n], f32) for n in NAMES]
    names = LOADED + LATE + ("res",)
    return pl.pallas_call(
        backward_kernel,
        out_shape=out_shapes,
        in_specs=[ANY] * (4 + len(names)) + [SM],
        out_specs=[ANY] * len(out_shapes),
        scratch_shapes=scratch,
        compiler_params=pltpu.CompilerParams(
            collective_id=1, has_side_effects=True, vmem_limit_bytes=67000000
        ),
    )(*weights, *[saved[n] for n in names], context)


def finish_kernel(gtok, output, g_qkv, g_out, g_up, g_down, vectors, *refs):
    ins = [gtok.at[0], gtok.at[1], output, g_qkv, g_out, g_up, g_down]
    o = refs[:6]
    outs = [o[1].at[0], o[1].at[1], o[0]] + list(o[2:6])
    b_up, biases, gains = refs[6:9]
    bufs = refs[9:16]
    sin, sout = refs[16:]
    loads = [pltpu.make_async_copy(ins[i], bufs[i], sin.at[i]) for i in range(7)]
    stores = [pltpu.make_async_copy(bufs[i], outs[i], sout.at[i]) for i in range(7)]
    for c in loads:
        c.start()
    z = lax.axis_index("narrow")
    rolled = pltpu.roll(vectors[0:8, :], (4 - z) % 4 * 32, 1)
    b_up[...] = vectors[8:9, :]
    biases[...] = rolled[0:6, 0:32]
    gains[...] = rolled[6:8, 0:32]
    for load, store in zip(loads, stores):
        load.wait()
        store.start()
    for c in stores:
        c.wait()


def finish(output, grad_tokens, vectors, *grads):
    dma = pltpu.SemaphoreType.DMA
    shape = jax.ShapeDtypeStruct
    big = [shape(a.shape, a.dtype) for a in (output, grad_tokens) + grads]
    bufs = [pltpu.VMEM(grad_tokens.shape[1:], f32)] * 2
    bufs += [pltpu.VMEM(a.shape, a.dtype) for a in (output,) + grads]
    return pl.pallas_call(
        finish_kernel,
        out_shape=big + [shape((1, 128), f32), shape((6, 32), f32), shape((2, 32), f32)],
        in_specs=[ANY] * 6 + [VM],
        out_specs=[ANY] * 6 + [VM] * 3,
        scratch_shapes=bufs + [dma((7,)), dma((7,))],
    )(grad_tokens, output, *grads, vectors)


def layer_shards(
    tokens, timestep, context, w_qkv, w_out, w_up, w_down, b_up, biases, gains, cotangent
):
    small = pack_vectors(b_up, biases, gains)
    shards = (small, w_qkv.transpose(1, 0, 2), w_out, w_up, w_down)
    results = forward(shards, tokens, cotangent, context, timestep)
    saved = dict(zip([name for name, _, _ in SAVED], results[4:]))
    output, grad_tokens, vectors, *grads = backward(results[:4], saved, context)
    done = finish(output, grad_tokens, vectors, *grads)
    output, grad_tokens, g_qkv, g_out, g_up, g_down, g_b_up, g_biases, g_gains = done
    return (
        output,
        grad_tokens,
        g_qkv.transpose(1, 0, 2),
        g_out,
        g_up,
        g_down,
        g_b_up.reshape(128),
        g_biases,
        g_gains,
    )


def solution(mesh):
    placed = (
        P("wide", "narrow", None),
        P("wide", None),
        P("wide", None),
        P("wide", None, "narrow"),
        P("narrow", "wide"),
        P("wide", "narrow"),
        P("narrow", "wide"),
        P(("wide", "narrow")),
        P(None, ("wide", "narrow")),
        P(None, ("wide", "narrow")),
        P("wide", "narrow", None),
    )
    by_item = mesh.shape["narrow"] == 4 and mesh.shape["wide"] == 8
    return jax.shard_map(
        layer_shards if by_item else shards,
        mesh=mesh,
        in_specs=placed,
        out_specs=(
            P("wide", "narrow", None),
            P("wide", "narrow", None),
            P("wide", None, "narrow"),
            P("narrow", "wide"),
            P("wide", "narrow"),
            P("narrow", "wide"),
            P(("wide", "narrow")),
            P(None, ("wide", "narrow")),
            P(None, ("wide", "narrow")),
        ),
        check_vma=False,
    )
```
